32 devices in a mesh: ta: 16 (over z, y, x), gz: 2 (over core).
Axes of the slice: x: 2, y: 2, z: 4, core: 2. Of those that a mesh axis runs over, the one named last changes fastest.
Arguments:
- time_links: float32 [2, 3, 3, 32, 8, 256], P(None, None, None, 'ta', 'gz'), may hold values from -1 to 1, as said below
- space_links: float32 [3, 2, 3, 3, 32, 8, 256], P(None, None, None, None, 'ta', 'gz'), may hold values from -1 to 1, as said below
Outputs:
- gauge: float32 [2, 3, 3, 32, 8, 256], P(None, None, None, 'ta', 'gz')
- links_fixed: float32 [3, 2, 3, 3, 32, 8, 256], P(None, None, None, None, 'ta', 'gz')
- action_profile: float32 [32, 8], P('ta', 'gz')
- action_mean: float32 [], replicated
The draws below stay inside these ranges and needn't reach their ends.
Inputs may be any that keep to these rules, and one draw needn't show every extreme that they name: `time_links`: every 3 x 3 complex matrix is unitary up to float32 rounding. `space_links`: every 3 x 3 complex matrix is unitary up to float32 rounding.
All inputs are finite; a program needn't handle non-finite values.
Results may differ from the reference program's by a relative error of at most 0.00024.
Values sent between devices are 32-bit elements; how exact they have to be, the bound alone decides.
No kernel may reach another device: no remote copies, remote signals or barrier semaphores. Data moves between devices by JAX's collectives and lax.ppermute only.
A program may use at most 64 MiB of HBM per device.

```python
import jax
import jax.numpy as jnp
from jax import lax

X = 16
Y = 16
NT = 32
NZ = 8


def matrix_product(first_pair, second_pair):
    first_real, first_imag = first_pair
    second_real, second_imag = second_pair
    real_part = jnp.sum(first_real[:, :, None] * second_real[None] - first_imag[:, :, None] * second_imag[None], axis=1)
    imag_part = jnp.sum(first_real[:, :, None] * second_imag[None] + first_imag[:, :, None] * second_real[None], axis=1)
    return (real_part, imag_part)


def embedded_block(first_row, second_row, theta, phi, psi):
    ones = jnp.ones_like(theta)
    zeros = jnp.zeros_like(theta)
    real_rows = [[ones if row == col else zeros for col in range(3)] for row in range(3)]
    imag_rows = [[zeros for col in range(3)] for row in range(3)]
    cosine = jnp.cos(theta)
    sine = jnp.sin(theta)
    real_rows[first_row][first_row] = cosine * jnp.cos(phi)
    imag_rows[first_row][first_row] = cosine * jnp.sin(phi)
    real_rows[first_row][second_row] = sine * jnp.cos(psi)
    imag_rows[first_row][second_row] = sine * jnp.sin(psi)
    real_rows[second_row][first_row] = -sine * jnp.cos(psi)
    imag_rows[second_row][first_row] = sine * jnp.sin(psi)
    real_rows[second_row][second_row] = cosine * jnp.cos(phi)
    imag_rows[second_row][second_row] = -cosine * jnp.sin(phi)
    real_part = jnp.stack([jnp.stack(row_list) for row_list in real_rows])
    imag_part = jnp.stack([jnp.stack(row_list) for row_list in imag_rows])
    return (real_part, imag_part)


def unitary_from_angles(angles):
    result = embedded_block(0, 1, angles[0], angles[1], angles[2])
    result = matrix_product(result, embedded_block(0, 2, angles[3], angles[4], angles[5]))
    result = matrix_product(result, embedded_block(1, 2, angles[6], angles[7], angles[8]))
    return jnp.stack([result[0], result[1]])


def draw_time_links(key, part):
    shape_all = (9, NT, NZ, X * Y)
    angles = 1.5 * jax.random.normal(key, shape_all, jnp.float32)
    return unitary_from_angles(angles)


def draw_space_links(key, part):
    shape_all = (3, 9, NT, NZ, X * Y)
    noise_key = jax.random.fold_in(key, 11)
    slice_key = jax.random.fold_in(key, 23)
    plane_key = jax.random.fold_in(key, 37)
    time_frac = (jnp.arange(NT, dtype=jnp.float32) / max(NT - 1, 1))[:, None, None]
    z_frac = (jnp.arange(NZ, dtype=jnp.float32) / max(NZ - 1, 1))[None, :, None]
    slice_factor = jnp.exp(jax.random.uniform(slice_key, (NT,), jnp.float32, -0.35, 0.35))[:, None, None]
    plane_factor = jnp.exp(jax.random.uniform(plane_key, (NZ,), jnp.float32, -0.2, 0.2))[None, :, None]
    wave = 1.0 + 0.3 * jnp.cos(6.2831853 * 3.0 * time_frac + 0.7)
    noise = jax.random.normal(noise_key, shape_all, jnp.float32)
    rise = (1.0 + z_frac) * jnp.sqrt(1.0 + 0.5 * time_frac)
    amplitude = 0.3 * rise * slice_factor * plane_factor * wave
    directions = []
    for direction in range(3):
        directions.append(unitary_from_angles(amplitude * noise[direction]))
    return jnp.stack(directions)


def setup_inputs(seed: int = 0) -> dict:
    seeds = jax.random.split(jax.random.key(seed), 3)
    return {
        "time_links": draw_time_links(jax.random.fold_in(seeds[2], 71), 0),
        "space_links": draw_space_links(jax.random.fold_in(seeds[2], 71), 0),
    }


def complex_product(first_pair, second_pair):
    first_real, first_imag = first_pair
    second_real, second_imag = second_pair
    real_part = jnp.sum(first_real[:, :, None] * second_real[None] - first_imag[:, :, None] * second_imag[None], axis=1)
    imag_part = jnp.sum(first_real[:, :, None] * second_imag[None] + first_imag[:, :, None] * second_real[None], axis=1)
    return real_part, imag_part


def dagger(matrix_pair):
    return jnp.swapaxes(matrix_pair[0], 0, 1), -jnp.swapaxes(matrix_pair[1], 0, 1)


def plane_step(matrix_pair, direction):
    def shifted(values):
        leading = values.shape[:-1]
        lattice_grid = values.reshape(leading + (X, Y))
        lattice_grid = jnp.roll(lattice_grid, -1, axis=lattice_grid.ndim - 2 + direction)
        return lattice_grid.reshape(leading + (X * Y,))
    return shifted(matrix_pair[0]), shifted(matrix_pair[1])


def roll_upward(matrix_pair):
    return jnp.roll(matrix_pair[0], -1, axis=-2), jnp.roll(matrix_pair[1], -1, axis=-2)


def plaquette_density(link_set, forward_x, forward_y):
    forward_z = [forward_x, forward_y]
    terms = []
    for first_dir, second_dir in ((0, 1), (0, 2), (1, 2)):
        along_first = link_set[first_dir]
        along_second = link_set[second_dir]
        second_moved = plane_step(along_second, first_dir)
        if second_dir < 2:
            first_moved = plane_step(along_first, second_dir)
        else:
            first_moved = forward_z[first_dir]
        loop_matrix = complex_product(complex_product(along_first, second_moved),
                                      complex_product(dagger(first_moved), dagger(along_second)))
        trace_real = loop_matrix[0][0, 0] + loop_matrix[0][1, 1] + loop_matrix[0][2, 2]
        terms.append(1.0 - trace_real / 3.0)
    return terms[0] + terms[1] + terms[2]


def reference(time_links, space_links):
    unit_real = jnp.broadcast_to(jnp.eye(3, dtype=jnp.float32)[:, :, None, None], (3, 3, NZ, X * Y))
    start_pair = (unit_real, jnp.zeros_like(unit_real))

    def advance(carry_pair, link_block):
        return complex_product(carry_pair, (link_block[0], link_block[1])), jnp.stack(carry_pair)

    unused_final, gauge_steps = lax.scan(advance, start_pair, jnp.moveaxis(time_links, 3, 0))
    gauge = jnp.moveaxis(gauge_steps, 0, 3)
    gauge_pair = (gauge[0], gauge[1])
    fixed = []
    for direction in range(3):
        link_pair = (space_links[direction, 0], space_links[direction, 1])
        if direction < 2:
            ahead = plane_step(gauge_pair, direction)
        else:
            ahead = roll_upward(gauge_pair)
        fixed.append(complex_product(complex_product(gauge_pair, link_pair), dagger(ahead)))
    links_fixed = jnp.stack([jnp.stack(pair) for pair in fixed])
    density = plaquette_density(fixed, roll_upward(fixed[0]), roll_upward(fixed[1]))
    action_profile = jnp.mean(density, axis=-1) / 3.0
    action_mean = jnp.mean(action_profile)
    return gauge, links_fixed, action_profile, action_mean
```

```python
import functools

import jax
import jax.numpy as jnp
from jax import lax
from jax.experimental import pallas as pl
from jax.experimental.pallas import tpu as pltpu
from jax.sharding import PartitionSpec as P

X = 16
Y = 16


VMEM = pl.BlockSpec(memory_space=pltpu.VMEM)
SMEM = pl.BlockSpec(memory_space=pltpu.SMEM)


def product(a, b):
    out = []
    for i in range(3):
        row = []
        for j in range(3):
            re = im = None
            for k in range(3):
                ar, ai = a[i][k]
                br, bi = b[k][j]
                r = ar * br - ai * bi
                m = ar * bi + ai * br
                re = r if re is None else re + r
                im = m if im is None else im + m
            row.append((re, im))
        out.append(row)
    return out


def product_dagger(a, b):
    out = []
    for i in range(3):
        row = []
        for j in range(3):
            re = im = None
            for k in range(3):
                ar, ai = a[i][k]
                br, bi = b[j][k]
                r = ar * br + ai * bi
                m = ai * br - ar * bi
                re = r if re is None else re + r
                im = m if im is None else im + m
            row.append((re, im))
        out.append(row)
    return out


def mapped(f, *mats):
    return [
        [tuple(f(*(m[i][j][c] for m in mats)) for c in range(2)) for j in range(3)]
        for i in range(3)
    ]


def load(ref, *tail):
    return [[tuple(ref[(c, i, j) + tail] for c in range(2)) for j in range(3)] for i in range(3)]


def store(ref, mat, *tail):
    for i in range(3):
        for j in range(3):
            for c in range(2):
                ref[(c, i, j) + tail] = mat[i][j][c]


def store_low(ref, mat):
    for i in range(3):
        for j in range(3):
            for c in range(2):
                ref[c, i, j] = mat[i][j][c][0:1, :]


def step_x(v):
    return pltpu.roll(v, v.shape[-1] - Y, v.ndim - 1)


def step_y(v):
    n = v.shape[-1]
    lane = lax.broadcasted_iota(jnp.int32, v.shape, v.ndim - 1)
    last = lax.rem(lane, Y) == Y - 1
    ahead = pltpu.roll(v, n - 1, v.ndim - 1)
    back = pltpu.roll(v, Y - 1, v.ndim - 1)
    return jnp.where(last, back, ahead)


def step_z(v, above):
    return jnp.concatenate([v[1:, :], above], axis=0)


def local_kernel(time_ref, out_ref):
    steps = time_ref.shape[3]
    run = load(time_ref, 0)
    for t in range(1, steps):
        run = product(run, load(time_ref, t))
    store(out_ref, run)


def combine_kernel(radix, has_before, low, digit_ref, *refs):
    slots = refs[:radix]
    refs = refs[radix:]
    before_ref = refs[0] if has_before else None
    outs = refs[1:] if has_before else refs
    total_ref, excl_ref = outs[0], outs[1]
    digit = digit_ref[0]
    for d in range(radix):

        @pl.when(digit == d)
        def _():
            run = None
            for j in range(radix):
                if j == d:
                    if run is None:
                        excl = load(before_ref) if has_before else None
                    else:
                        excl = product(run, load(before_ref)) if has_before else run
                    if excl is None:
                        one = jnp.ones(excl_ref.shape[3:], jnp.float32)
                        zero = jnp.zeros_like(one)
                        excl = [[(one if a == b else zero, zero) for b in range(3)] for a in range(3)]
                    store(excl_ref, excl)
                    if low:
                        store_low(outs[3], excl)
                piece = load(slots[j ^ d])
                run = piece if run is None else product(run, piece)
            store(total_ref, run)
            if low:
                store_low(outs[2], run)


def plaquette_kernel(space_ref, above_ref, profile_ref, total_ref):
    steps, layers = space_ref.shape[4], space_ref.shape[5]
    sites = space_ref.shape[6]
    eye = (
        lax.broadcasted_iota(jnp.int32, (layers, layers), 0)
        == lax.broadcasted_iota(jnp.int32, (layers, layers), 1)
    )
    whole = jnp.zeros((1, 1), jnp.float32)
    for t in range(steps):
        links = [load(space_ref.at[mu], t) for mu in range(3)]
        above = [load(above_ref.at[mu], t) for mu in range(2)]

        def moved(mu, nu):
            if nu == 0:
                return mapped(step_x, links[mu])
            if nu == 1:
                return mapped(step_y, links[mu])
            return mapped(step_z, links[mu], above[mu])

        density = None
        for mu, nu in ((0, 1), (0, 2), (1, 2)):
            left = product(links[mu], moved(nu, mu))
            right = product(links[nu], moved(mu, nu))
            trace = None
            for i in range(3):
                for j in range(3):
                    term = left[i][j][0] * right[i][j][0] + left[i][j][1] * right[i][j][1]
                    trace = term if trace is None else trace + term
            term = 1.0 - trace / 3.0
            density = term if density is None else density + term
        prof = jnp.sum(density, axis=1, keepdims=True) / (3.0 * sites)
        row = jnp.sum(jnp.where(eye, jnp.broadcast_to(prof, (layers, layers)), 0.0), axis=0, keepdims=True)
        profile_ref[t : t + 1, :] = row
        whole = whole + jnp.sum(row, axis=1, keepdims=True)
    total_ref[...] = jnp.broadcast_to(whole, total_ref.shape)


def final_kernel(radix, digit_ref, excl_ref, excl_up_ref, *refs):
    got = refs[: radix - 1]
    got_up = refs[radix - 1 : 2 * radix - 2]
    time_ref, time_up_ref, space_ref, gauge_ref, fixed_ref, up_ref = refs[2 * radix - 2 :]
    steps = time_ref.shape[3]
    digit = digit_ref[0]
    for d in range(radix):

        @pl.when(digit == d)
        def _():
            run = load(excl_ref)
            run_up = load(excl_up_ref)
            for k in range(d):
                run = product(load(got[k]), run)
                run_up = product(load(got_up[k]), run_up)
            store(gauge_ref, run, 0)
            store(up_ref, run_up)

    for t in range(steps):
        gauge = load(gauge_ref, t)
        above = load(up_ref)
        if t + 1 < steps:
            store(gauge_ref, product(gauge, load(time_ref, t)), t + 1)
            store(up_ref, product(above, load(time_up_ref, t)))
        for mu in range(3):
            if mu == 0:
                ahead = mapped(step_x, gauge)
            elif mu == 1:
                ahead = mapped(step_y, gauge)
            else:
                ahead = mapped(step_z, gauge, above)
            fixed = product_dagger(product(gauge, load(space_ref.at[mu], t)), ahead)
            store(fixed_ref.at[mu], fixed, t)


def call(kernel, out_shapes, n_in, smem=0, scratch=()):
    return pl.pallas_call(
        kernel,
        out_shape=[jax.ShapeDtypeStruct(s, jnp.float32) for s in out_shapes],
        in_specs=[SMEM] * smem + [VMEM] * (n_in - smem),
        out_specs=[VMEM] * len(out_shapes),
        scratch_shapes=list(scratch),
    )


def bit_groups(count, width):
    first = count % width
    sizes = ([first] if first else []) + [width] * (count // width)
    groups, at = [], 0
    for size in sizes:
        groups.append((at, size))
        at += size
    return groups


def make_on_device(n_ta, n_gz):
    both = ("ta", "gz")

    def xor_exchange(value, axis, count, at, size):
        return [value] + [
            lax.ppermute(value, axis, [(i, i ^ (m << at)) for i in range(count)])
            for m in range(1, 1 << size)
        ]

    def from_upper(value):
        return lax.ppermute(value, "gz", [((g + 1) % n_gz, g) for g in range(n_gz)])

    def on_device(time_links, space_links):
        steps, layers, sites = time_links.shape[3:]
        mat = (2, 3, 3, layers, sites)
        low = (2, 3, 3, 1, sites)
        me = lax.axis_index("ta")

        total = call(local_kernel, [mat], 1)(time_links)[0]
        excl = None
        groups = bit_groups(n_ta.bit_length() - 1, 2)
        for at, size in groups[:-1]:
            slots = xor_exchange(total, "ta", n_ta, at, size)
            digit = ((me >> at) & ((1 << size) - 1)).reshape(1)
            is_last = (at, size) == groups[-2]
            kernel = functools.partial(combine_kernel, 1 << size, excl is not None, is_last)
            args = [digit] + slots + ([excl] if excl is not None else [])
            outs = call(kernel, [mat, mat] + ([low, low] if is_last else []), len(args), 1)(*args)
            total, excl = outs[0], outs[1]
            if is_last:
                total_low, excl_low = outs[2], outs[3]

        at, size = groups[-1]
        radix = 1 << size
        digit = ((me >> at) & (radix - 1)).reshape(1)
        got, got_up = [], []
        for k in range(1, radix):
            pairs = [(i - (k << at), i) for i in range(n_ta) if ((i >> at) & (radix - 1)) >= k]
            got.append(lax.ppermute(total, "ta", pairs))
            up_pairs = [(s * n_gz + (g + 1) % n_gz, i * n_gz + g) for s, i in pairs for g in range(n_gz)]
            got_up.append(lax.ppermute(total_low, both, up_pairs))
        excl_up = from_upper(excl_low)
        time_up = from_upper(time_links[..., 0:1, :])
        args = [digit, excl, excl_up] + got + got_up + [time_links, time_up, space_links]
        gauge, fixed = call(
            functools.partial(final_kernel, radix),
            [time_links.shape, space_links.shape],
            len(args),
            1,
            [pltpu.VMEM(low, jnp.float32)],
        )(*args)

        space_up = from_upper(space_links[0:2, ..., 0:1, :])
        profile, part = call(plaquette_kernel, [(steps, layers), (1, 128)], 2)(space_links, space_up)
        count = n_ta * n_gz
        for at, size in bit_groups(count.bit_length() - 1, 3):
            parts = xor_exchange(part, both, count, at, size)
            while len(parts) > 1:
                parts = [parts[i] + parts[i + 1] for i in range(0, len(parts), 2)]
            part = parts[0]
        mean = part[0, 0] / (steps * layers * count)
        return gauge, fixed, profile, mean

    return on_device


def solution(mesh):
    return jax.shard_map(
        make_on_device(mesh.shape["ta"], mesh.shape["gz"]),
        mesh=mesh,
        in_specs=(
            P(None, None, None, "ta", "gz", None),
            P(None, None, None, None, "ta", "gz", None),
        ),
        out_specs=(
            P(None, None, None, "ta", "gz", None),
            P(None, None, None, None, "ta", "gz", None),
            P("ta", "gz"),
            P(),
        ),
        check_vma=False,
    )
```

```python
import functools

import jax
import jax.numpy as jnp
from jax import lax
from jax.experimental import pallas as pl
from jax.experimental.pallas import tpu as pltpu
from jax.sharding import PartitionSpec as P

X = 16
Y = 16


VMEM = pl.BlockSpec(memory_space=pltpu.VMEM)
SMEM = pl.BlockSpec(memory_space=pltpu.SMEM)


def product(a, b):
    out = []
    for i in range(3):
        row = []
        for j in range(3):
            re = im = None
            for k in range(3):
                ar, ai = a[i][k]
                br, bi = b[k][j]
                r = ar * br - ai * bi
                m = ar * bi + ai * br
                re = r if re is None else re + r
                im = m if im is None else im + m
            row.append((re, im))
        out.append(row)
    return out


def product_dagger(a, b):
    out = []
    for i in range(3):
        row = []
        for j in range(3):
            re = im = None
            for k in range(3):
                ar, ai = a[i][k]
                br, bi = b[j][k]
                r = ar * br + ai * bi
                m = ai * br - ar * bi
                re = r if re is None else re + r
                im = m if im is None else im + m
            row.append((re, im))
        out.append(row)
    return out


def mapped(f, *mats):
    return [
        [tuple(f(*(m[i][j][c] for m in mats)) for c in range(2)) for j in range(3)]
        for i in range(3)
    ]


def load(ref, *tail):
    return [[tuple(ref[(c, i, j) + tail] for c in range(2)) for j in range(3)] for i in range(3)]


def store(ref, mat, *tail):
    for i in range(3):
        for j in range(3):
            for c in range(2):
                ref[(c, i, j) + tail] = mat[i][j][c]


def store_low(ref, mat):
    for i in range(3):
        for j in range(3):
            for c in range(2):
                ref[c, i, j] = mat[i][j][c][0:1, :]


def step_x(v):
    return pltpu.roll(v, v.shape[-1] - Y, v.ndim - 1)


def step_y(v):
    n = v.shape[-1]
    lane = lax.broadcasted_iota(jnp.int32, v.shape, v.ndim - 1)
    last = lax.rem(lane, Y) == Y - 1
    ahead = pltpu.roll(v, n - 1, v.ndim - 1)
    back = pltpu.roll(v, Y - 1, v.ndim - 1)
    return jnp.where(last, back, ahead)


def step_z(v, above):
    return jnp.concatenate([v[1:, :], above], axis=0)


def local_kernel(time_ref, out_ref):
    steps = time_ref.shape[3]
    run = load(time_ref, 0)
    for t in range(1, steps):
        run = product(run, load(time_ref, t))
    store(out_ref, run)


def low_kernel(time_ref, space_ref, low_ref):
    low_ref[0] = time_ref[..., 0:1, :]
    low_ref[1:3] = space_ref[0:2, ..., 0:1, :]


def combine_kernel(has_before, low, bit_ref, mine_ref, other_ref, *refs):
    before_ref = refs[0] if has_before else None
    outs = refs[1:] if has_before else refs
    total_ref, excl_ref = outs[0], outs[1]
    upper = bit_ref[0] == 1

    def finish(total, excl):
        store(total_ref, total)
        store(excl_ref, excl)
        if low:
            store_low(outs[2], total)
            store_low(outs[3], excl)

    @pl.when(upper)
    def _():
        other = load(other_ref)
        excl = product(other, load(before_ref)) if has_before else other
        finish(product(other, load(mine_ref)), excl)

    @pl.when(jnp.logical_not(upper))
    def _():
        if has_before:
            excl = load(before_ref)
        else:
            one = jnp.ones(excl_ref.shape[3:], jnp.float32)
            zero = jnp.zeros_like(one)
            excl = [[(one if a == b else zero, zero) for b in range(3)] for a in range(3)]
        finish(product(load(mine_ref), load(other_ref)), excl)


def plaquette_kernel(space_ref, above_ref, profile_ref, total_ref):
    steps, layers = space_ref.shape[4], space_ref.shape[5]
    sites = space_ref.shape[6]
    eye = (
        lax.broadcasted_iota(jnp.int32, (layers, layers), 0)
        == lax.broadcasted_iota(jnp.int32, (layers, layers), 1)
    )
    whole = jnp.zeros((1, 1), jnp.float32)
    for t in range(steps):
        links = [load(space_ref.at[mu], t) for mu in range(3)]
        above = [load(above_ref.at[mu + 1], t) for mu in range(2)]

        def moved(mu, nu):
            if nu == 0:
                return mapped(step_x, links[mu])
            if nu == 1:
                return mapped(step_y, links[mu])
            return mapped(step_z, links[mu], above[mu])

        density = None
        for mu, nu in ((0, 1), (0, 2), (1, 2)):
            left = product(links[mu], moved(nu, mu))
            right = product(links[nu], moved(mu, nu))
            trace = None
            for i in range(3):
                for j in range(3):
                    term = left[i][j][0] * right[i][j][0] + left[i][j][1] * right[i][j][1]
                    trace = term if trace is None else trace + term
            term = 1.0 - trace / 3.0
            density = term if density is None else density + term
        prof = jnp.sum(density, axis=1, keepdims=True) / (3.0 * sites)
        row = jnp.sum(jnp.where(eye, jnp.broadcast_to(prof, (layers, layers)), 0.0), axis=0, keepdims=True)
        profile_ref[t : t + 1, :] = row
        whole = whole + jnp.sum(row, axis=1, keepdims=True)
    total_ref[...] = jnp.broadcast_to(whole, total_ref.shape)


def final_kernel(
    bit_ref, excl_ref, excl_up_ref, got_ref, got_up_ref, time_ref, time_up_ref, space_ref,
    gauge_ref, fixed_ref, up_ref,
):
    steps = time_ref.shape[3]
    upper = bit_ref[0] == 1

    @pl.when(upper)
    def _():
        store(gauge_ref, product(load(got_ref), load(excl_ref)), 0)
        store(up_ref, product(load(got_up_ref), load(excl_up_ref)))

    @pl.when(jnp.logical_not(upper))
    def _():
        store(gauge_ref, load(excl_ref), 0)
        store(up_ref, load(excl_up_ref))

    for t in range(steps):
        gauge = load(gauge_ref, t)
        above = load(up_ref)
        if t + 1 < steps:
            store(gauge_ref, product(gauge, load(time_ref, t)), t + 1)
            store(up_ref, product(above, load(time_up_ref.at[0], t)))
        for mu in range(3):
            if mu == 0:
                ahead = mapped(step_x, gauge)
            elif mu == 1:
                ahead = mapped(step_y, gauge)
            else:
                ahead = mapped(step_z, gauge, above)
            fixed = product_dagger(product(gauge, load(space_ref.at[mu], t)), ahead)
            store(fixed_ref.at[mu], fixed, t)


def call(kernel, out_shapes, args, smem=0, scratch=(), keep=()):
    return pl.pallas_call(
        kernel,
        out_shape=[
            pltpu.VMEM(s, jnp.float32) if i in keep else jax.ShapeDtypeStruct(s, jnp.float32)
            for i, s in enumerate(out_shapes)
        ],
        in_specs=[SMEM] * smem + [VMEM] * (len(args) - smem),
        out_specs=[VMEM] * len(out_shapes),
        scratch_shapes=list(scratch),
    )(*args)


def near(value):
    return pltpu.with_memory_space_constraint(value, pltpu.VMEM)


def make_on_device(n_ta, n_gz):
    both = ("ta", "gz")
    count = n_ta * n_gz
    bits = n_ta.bit_length() - 1

    def swap(value, axis, n, mask):
        return lax.ppermute(value, axis, [(i, i ^ mask) for i in range(n)])

    def from_upper(value, mask=0):
        pairs = [
            ((i ^ mask) * n_gz + (g + 1) % n_gz, i * n_gz + g) for i in range(n_ta) for g in range(n_gz)
        ]
        return lax.ppermute(value, both, pairs)

    def on_device(time_links, space_links):
        steps, layers, sites = time_links.shape[3:]
        mat = (2, 3, 3, layers, sites)
        low = (2, 3, 3, 1, sites)
        me = lax.axis_index("ta")

        def bit(at):
            return ((me >> at) & 1).reshape(1)

        def after(value, *others):
            return lax.optimization_barrier((value,) + others)[0]

        def summed(part, masks):
            parts = [part, swap(part, both, count, masks[0]), swap(part, both, count, masks[1])]
            parts.append(swap(part, both, count, masks[0] ^ masks[1]))
            return (parts[0] + parts[1]) + (parts[2] + parts[3])

        total = call(local_kernel, [mat], [time_links], keep=(0,))[0]
        excl = None
        part = None
        left = [1 << at for at in range(count.bit_length() - 1)]
        for at in range(bits - 1):
            other = swap(total, "ta", n_ta, 1 << at)
            is_last = at == bits - 2
            if at == 0:
                lows = call(
                    low_kernel,
                    [(3,) + time_links.shape[:4] + (1, sites)],
                    [time_links, space_links],
                    keep=(0,),
                )[0]
                lows_up = from_upper(lows)
                other = after(other, lows_up)
            elif at == 1:
                profile, part = call(
                    plaquette_kernel,
                    [(steps, layers), (1, 128)],
                    [space_links, near(lows_up)],
                    keep=(1,),
                )
                other = after(other, part)
            else:
                part = summed(part, left[:2])
                left = left[2:]
                other = after(other, part)
            args = [bit(at), near(total), near(other)] + ([near(excl)] if excl is not None else [])
            outs = call(
                functools.partial(combine_kernel, excl is not None, is_last),
                [mat, mat] + ([low, low] if is_last else []),
                args,
                1,
                keep=range(4),
            )
            total, excl = outs[0], outs[1]
        total_low, excl_low = outs[2], outs[3]
        top = 1 << (bits - 1)
        got = swap(total, "ta", n_ta, top)
        got_up = from_upper(total_low, top)
        excl_up = from_upper(excl_low)
        while len(left) > 1:
            part = summed(part, left[:2])
            left = left[2:]
        got = after(got, part)
        for mask in left:
            part = part + swap(part, both, count, mask)
        args = [bit(bits - 1)] + [near(v) for v in (excl, excl_up, got, got_up)]
        args += [time_links, near(lows_up), space_links]
        gauge, fixed = call(
            final_kernel,
            [time_links.shape, space_links.shape],
            args,
            1,
            [pltpu.VMEM(low, jnp.float32)],
        )
        mean = part[0, 0] / (steps * layers * count)
        return gauge, fixed, profile, mean

    return on_device


def solution(mesh):
    return jax.shard_map(
        make_on_device(mesh.shape["ta"], mesh.shape["gz"]),
        mesh=mesh,
        in_specs=(
            P(None, None, None, "ta", "gz", None),
            P(None, None, None, None, "ta", "gz", None),
        ),
        out_specs=(
            P(None, None, None, "ta", "gz", None),
            P(None, None, None, None, "ta", "gz", None),
            P("ta", "gz"),
            P(),
        ),
        check_vma=False,
    )
```

```python
import functools

import jax
import jax.numpy as jnp
from jax import lax
from jax.experimental import pallas as pl
from jax.experimental.pallas import tpu as pltpu
from jax.sharding import PartitionSpec as P


Y = 16


VMEM = pl.BlockSpec(memory_space=pltpu.VMEM)
SMEM = pl.BlockSpec(memory_space=pltpu.SMEM)


def product(a, b):
    out = []
    for i in range(3):
        row = []
        for j in range(3):
            re = im = None
            for k in range(3):
                ar, ai = a[i][k]
                br, bi = b[k][j]
                r = ar * br - ai * bi
                m = ar * bi + ai * br
                re = r if re is None else re + r
                im = m if im is None else im + m
            row.append((re, im))
        out.append(row)
    return out


def product_dagger(a, b):
    out = []
    for i in range(3):
        row = []
        for j in range(3):
            re = im = None
            for k in range(3):
                ar, ai = a[i][k]
                br, bi = b[j][k]
                r = ar * br + ai * bi
                m = ai * br - ar * bi
                re = r if re is None else re + r
                im = m if im is None else im + m
            row.append((re, im))
        out.append(row)
    return out


def mapped(f, *mats):
    return [
        [tuple(f(*(m[i][j][c] for m in mats)) for c in range(2)) for j in range(3)]
        for i in range(3)
    ]


def load(ref, *tail):
    return [[tuple(ref[(c, i, j) + tail] for c in range(2)) for j in range(3)] for i in range(3)]


def store(ref, mat, *tail):
    for i in range(3):
        for j in range(3):
            for c in range(2):
                ref[(c, i, j) + tail] = mat[i][j][c]


def store_low(ref, mat):
    for i in range(3):
        for j in range(3):
            for c in range(2):
                ref[c, i, j] = mat[i][j][c][0:1, :]


def step_x(v):
    return pltpu.roll(v, v.shape[-1] - Y, v.ndim - 1)


def step_y(v):
    n = v.shape[-1]
    lane = lax.broadcasted_iota(jnp.int32, v.shape, v.ndim - 1)
    last = lax.rem(lane, Y) == Y - 1
    ahead = pltpu.roll(v, n - 1, v.ndim - 1)
    back = pltpu.roll(v, Y - 1, v.ndim - 1)
    return jnp.where(last, back, ahead)


def step_z(v, above):
    return jnp.concatenate([v[1:, :], above], axis=0)


def first_kernel(time_ref, space_ref, out_ref, low_ref):
    steps = time_ref.shape[3]
    run = load(time_ref, 0)
    for t in range(1, steps):
        run = product(run, load(time_ref, t))
    store(out_ref, run)
    low_ref[0] = time_ref[..., 0:1, :]
    low_ref[1:3] = space_ref[0:2, ..., 0:1, :]


def group_kernel(radix, digit_ref, *refs):
    slots = refs[:radix]
    total_ref, excl_ref = refs[radix:]
    digit = digit_ref[0]
    for d in range(radix):

        @pl.when(digit == d)
        def _():
            run = None
            for j in range(radix):
                if j == d:
                    if run is None:
                        one = jnp.ones(excl_ref.shape[3:], jnp.float32)
                        zero = jnp.zeros_like(one)
                        excl = [[(one if a == b else zero, zero) for b in range(3)] for a in range(3)]
                        store(excl_ref, excl)
                    else:
                        store(excl_ref, run)
                piece = load(slots[j ^ d])
                run = piece if run is None else product(run, piece)
            store(total_ref, run)


def combine_kernel(has_before, low, bit_ref, mine_ref, other_ref, *refs):
    before_ref = refs[0] if has_before else None
    outs = refs[1:] if has_before else refs
    total_ref, excl_ref = outs[0], outs[1]
    upper = bit_ref[0] == 1

    def finish(total, excl):
        store(total_ref, total)
        store(excl_ref, excl)
        if low:
            store_low(outs[2], total)
            store_low(outs[3], excl)

    @pl.when(upper)
    def _():
        other = load(other_ref)
        excl = product(other, load(before_ref)) if has_before else other
        finish(product(other, load(mine_ref)), excl)

    @pl.when(jnp.logical_not(upper))
    def _():
        if has_before:
            excl = load(before_ref)
        else:
            one = jnp.ones(excl_ref.shape[3:], jnp.float32)
            zero = jnp.zeros_like(one)
            excl = [[(one if a == b else zero, zero) for b in range(3)] for a in range(3)]
        finish(product(load(mine_ref), load(other_ref)), excl)


def plaquette_kernel(space_ref, above_ref, profile_ref, total_ref):
    steps, layers = space_ref.shape[4], space_ref.shape[5]
    sites = space_ref.shape[6]
    eye = (
        lax.broadcasted_iota(jnp.int32, (layers, layers), 0)
        == lax.broadcasted_iota(jnp.int32, (layers, layers), 1)
    )
    whole = jnp.zeros((1, 1), jnp.float32)
    for t in range(steps):
        links = [load(space_ref.at[mu], t) for mu in range(3)]
        above = [load(above_ref.at[mu + 1], t) for mu in range(2)]

        def moved(mu, nu):
            if nu == 0:
                return mapped(step_x, links[mu])
            if nu == 1:
                return mapped(step_y, links[mu])
            return mapped(step_z, links[mu], above[mu])

        density = None
        for mu, nu in ((0, 1), (0, 2), (1, 2)):
            left = product(links[mu], moved(nu, mu))
            right = product(links[nu], moved(mu, nu))
            trace = None
            for i in range(3):
                for j in range(3):
                    term = left[i][j][0] * right[i][j][0] + left[i][j][1] * right[i][j][1]
                    trace = term if trace is None else trace + term
            term = 1.0 - trace / 3.0
            density = term if density is None else density + term
        prof = jnp.sum(density, axis=1, keepdims=True) / (3.0 * sites)
        row = jnp.sum(jnp.where(eye, jnp.broadcast_to(prof, (layers, layers)), 0.0), axis=0, keepdims=True)
        profile_ref[t : t + 1, :] = row
        whole = whole + jnp.sum(row, axis=1, keepdims=True)
    total_ref[...] = jnp.broadcast_to(whole, total_ref.shape)


def final_kernel(
    bit_ref, excl_ref, excl_up_ref, got_ref, got_up_ref, time_ref, time_up_ref, space_ref,
    gauge_ref, fixed_ref, up_ref,
):
    steps = time_ref.shape[3]
    upper = bit_ref[0] == 1

    @pl.when(upper)
    def _():
        store(gauge_ref, product(load(got_ref), load(excl_ref)), 0)
        store(up_ref, product(load(got_up_ref), load(excl_up_ref)))

    @pl.when(jnp.logical_not(upper))
    def _():
        store(gauge_ref, load(excl_ref), 0)
        store(up_ref, load(excl_up_ref))

    for t in range(steps):
        gauge = load(gauge_ref, t)
        above = load(up_ref)
        if t + 1 < steps:
            store(gauge_ref, product(gauge, load(time_ref, t)), t + 1)
            store(up_ref, product(above, load(time_up_ref.at[0], t)))
        for mu in range(3):
            if mu == 0:
                ahead = mapped(step_x, gauge)
            elif mu == 1:
                ahead = mapped(step_y, gauge)
            else:
                ahead = mapped(step_z, gauge, above)
            fixed = product_dagger(product(gauge, load(space_ref.at[mu], t)), ahead)
            store(fixed_ref.at[mu], fixed, t)


def call(kernel, out_shapes, args, smem=0, scratch=(), keep=()):
    return pl.pallas_call(
        kernel,
        out_shape=[
            pltpu.VMEM(s, jnp.float32) if i in keep else jax.ShapeDtypeStruct(s, jnp.float32)
            for i, s in enumerate(out_shapes)
        ],
        in_specs=[SMEM] * smem + [VMEM] * (len(args) - smem),
        out_specs=[VMEM] * len(out_shapes),
        scratch_shapes=list(scratch),
    )(*args)


def near(value):
    return pltpu.with_memory_space_constraint(value, pltpu.VMEM)


def make_on_device(n_ta, n_gz):
    both = ("ta", "gz")
    count = n_ta * n_gz
    bits = n_ta.bit_length() - 1

    def swap(value, axis, n, mask):
        return lax.ppermute(value, axis, [(i, i ^ mask) for i in range(n)])

    def from_upper(value, mask=0):
        pairs = [
            ((i ^ mask) * n_gz + (g + 1) % n_gz, i * n_gz + g) for i in range(n_ta) for g in range(n_gz)
        ]
        return lax.ppermute(value, both, pairs)

    def on_device(time_links, space_links):
        return body(time_links, space_links)

    def body(time_links, space_links):
        steps, layers, sites = time_links.shape[3:]
        mat = (2, 3, 3, layers, sites)
        low = (2, 3, 3, 1, sites)
        me = lax.axis_index("ta")

        def bit(at):
            return ((me >> at) & 1).reshape(1)

        def after(value, *others):
            return lax.optimization_barrier((value,) + others)[0]

        def summed(part, masks):
            parts = [part, swap(part, both, count, masks[0]), swap(part, both, count, masks[1])]
            parts.append(swap(part, both, count, masks[0] ^ masks[1]))
            return (parts[0] + parts[1]) + (parts[2] + parts[3])

        total, lows = call(
            first_kernel,
            [mat, (3,) + time_links.shape[:4] + (1, sites)],
            [time_links, space_links],
            keep=(0, 1),
        )
        slots = [total]
        for mask in (1, 2, 3):
            slots.append(swap(total, "ta", n_ta, mask))
        lows_up = from_upper(lows)
        profile, part = call(
            plaquette_kernel,
            [(steps, layers), (1, 128)],
            [space_links, near(lows_up)],
            keep=(1,),
        )
        args = [(me & 3).reshape(1)] + [near(v) for v in slots]
        total, excl = call(
            functools.partial(group_kernel, 4), [mat, mat], args, 1, keep=range(2)
        )
        left = [1 << at for at in range(count.bit_length() - 1)]
        for at in range(2, bits - 1):
            other = swap(total, "ta", n_ta, 1 << at)
            is_last = at == bits - 2
            if at == 2:
                part = summed(part, left[:2])
                left = left[2:]
                other = after(other, part)
            args = [bit(at)] + [near(v) for v in (total, other, excl)]
            outs = call(
                functools.partial(combine_kernel, True, is_last),
                [mat, mat] + ([low, low] if is_last else []),
                args,
                1,
                keep=range(4),
            )
            total, excl = outs[0], outs[1]
        total_low, excl_low = outs[2], outs[3]
        top = 1 << (bits - 1)
        got = swap(total, "ta", n_ta, top)
        got_up = from_upper(total_low, top)
        excl_up = from_upper(excl_low)
        while len(left) > 1:
            part = summed(part, left[:2])
            left = left[2:]
        got = after(got, part)
        for mask in left:
            more = swap(part, both, count, mask)
            part = part + more
        args = [bit(bits - 1)] + [near(v) for v in (excl, excl_up, got, got_up)]
        args += [time_links, near(lows_up), space_links]
        gauge, fixed = call(
            final_kernel,
            [time_links.shape, space_links.shape],
            args,
            1,
            [pltpu.VMEM(low, jnp.float32)],
        )
        mean = part[0, 0] / (steps * layers * count)
        return gauge, fixed, profile, mean

    return on_device


def solution(mesh):
    return jax.shard_map(
        make_on_device(mesh.shape["ta"], mesh.shape["gz"]),
        mesh=mesh,
        in_specs=(
            P(None, None, None, "ta", "gz", None),
            P(None, None, None, None, "ta", "gz", None),
        ),
        out_specs=(
            P(None, None, None, "ta", "gz", None),
            P(None, None, None, None, "ta", "gz", None),
            P("ta", "gz"),
            P(),
        ),
        check_vma=False,
    )
```

```python
import functools

import jax
import jax.numpy as jnp
from jax import lax
from jax.experimental import pallas as pl
from jax.experimental.pallas import tpu as pltpu
from jax.sharding import PartitionSpec as P


Y = 16


VMEM = pl.BlockSpec(memory_space=pltpu.VMEM)
SMEM = pl.BlockSpec(memory_space=pltpu.SMEM)


def product(a, b):
    out = []
    for i in range(3):
        row = []
        for j in range(3):
            re = im = None
            for k in range(3):
                ar, ai = a[i][k]
                br, bi = b[k][j]
                r = ar * br - ai * bi
                m = ar * bi + ai * br
                re = r if re is None else re + r
                im = m if im is None else im + m
            row.append((re, im))
        out.append(row)
    return out


def product_dagger(a, b):
    out = []
    for i in range(3):
        row = []
        for j in range(3):
            re = im = None
            for k in range(3):
                ar, ai = a[i][k]
                br, bi = b[j][k]
                r = ar * br + ai * bi
                m = ai * br - ar * bi
                re = r if re is None else re + r
                im = m if im is None else im + m
            row.append((re, im))
        out.append(row)
    return out


def mapped(f, *mats):
    return [
        [tuple(f(*(m[i][j][c] for m in mats)) for c in range(2)) for j in range(3)]
        for i in range(3)
    ]


def load(ref, *tail):
    return [[tuple(ref[(c, i, j) + tail] for c in range(2)) for j in range(3)] for i in range(3)]


def store(ref, mat, *tail):
    for i in range(3):
        for j in range(3):
            for c in range(2):
                ref[(c, i, j) + tail] = mat[i][j][c]


def store_low(ref, mat):
    for i in range(3):
        for j in range(3):
            for c in range(2):
                ref[c, i, j] = mat[i][j][c][0:1, :]


def times(a, b):
    return a[0] * b[0] - a[1] * b[1], a[0] * b[1] + a[1] * b[0]


def cross(mat):
    out = []
    for j in range(3):
        k, m = (j + 1) % 3, (j + 2) % 3
        p = times(mat[0][k], mat[1][m])
        q = times(mat[0][m], mat[1][k])
        out.append((p[0] - q[0], p[1] - q[1]))
    return out


def pack(ref, mat):
    for i in range(2):
        for j in range(3):
            for c in range(2):
                ref[i * 6 + j * 2 + c] = mat[i][j][c]
    terms = [times(mat[2][j], v) for j, v in enumerate(cross(mat))]
    for c in range(2):
        ref[12 + c] = terms[0][c] + terms[1][c] + terms[2][c]


def unpack(ref):
    rows = [
        [tuple(ref[i * 6 + j * 2 + c] for c in range(2)) for j in range(3)] for i in range(2)
    ]
    det = (ref[12], ref[13])
    rows.append([times(det, (v[0], -v[1])) for v in cross(rows)])
    return rows


def step_x(v):
    return pltpu.roll(v, v.shape[-1] - Y, v.ndim - 1)


def step_y(v):
    n = v.shape[-1]
    lane = lax.broadcasted_iota(jnp.int32, v.shape, v.ndim - 1)
    last = lax.rem(lane, Y) == Y - 1
    ahead = pltpu.roll(v, n - 1, v.ndim - 1)
    back = pltpu.roll(v, Y - 1, v.ndim - 1)
    return jnp.where(last, back, ahead)


def step_z(v, above):
    return jnp.concatenate([v[1:, :], above], axis=0)


def first_kernel(time_ref, space_ref, out_ref, low_ref):
    steps = time_ref.shape[3]
    run = load(time_ref, 0)
    for t in range(1, steps):
        run = product(run, load(time_ref, t))
    pack(out_ref, run)
    low_ref[0] = time_ref[..., 0:1, :]
    low_ref[1:3] = space_ref[0:2, ..., 0:1, :]


def group_kernel(radix, digit_ref, *refs):
    slots = refs[:radix]
    total_ref, excl_ref = refs[radix:]
    digit = digit_ref[0]
    for d in range(radix):

        @pl.when(digit == d)
        def _():
            run = None
            for j in range(radix):
                if j == d:
                    if run is None:
                        one = jnp.ones(excl_ref.shape[3:], jnp.float32)
                        zero = jnp.zeros_like(one)
                        excl = [[(one if a == b else zero, zero) for b in range(3)] for a in range(3)]
                        store(excl_ref, excl)
                    else:
                        store(excl_ref, run)
                piece = unpack(slots[j ^ d])
                run = piece if run is None else product(run, piece)
            pack(total_ref, run)


def combine_kernel(has_before, low, bit_ref, mine_ref, other_ref, *refs):
    before_ref = refs[0] if has_before else None
    outs = refs[1:] if has_before else refs
    total_ref, excl_ref = outs[0], outs[1]
    upper = bit_ref[0] == 1

    def finish(total, excl):
        pack(total_ref, total)
        store(excl_ref, excl)
        if low:
            store_low(outs[2], total)
            store_low(outs[3], excl)

    @pl.when(upper)
    def _():
        other = unpack(other_ref)
        excl = product(other, load(before_ref)) if has_before else other
        finish(product(other, unpack(mine_ref)), excl)

    @pl.when(jnp.logical_not(upper))
    def _():
        if has_before:
            excl = load(before_ref)
        else:
            one = jnp.ones(excl_ref.shape[3:], jnp.float32)
            zero = jnp.zeros_like(one)
            excl = [[(one if a == b else zero, zero) for b in range(3)] for a in range(3)]
        finish(product(unpack(mine_ref), unpack(other_ref)), excl)


def plaquette_kernel(space_ref, above_ref, profile_ref, total_ref):
    steps, layers = space_ref.shape[4], space_ref.shape[5]
    sites = space_ref.shape[6]
    eye = (
        lax.broadcasted_iota(jnp.int32, (layers, layers), 0)
        == lax.broadcasted_iota(jnp.int32, (layers, layers), 1)
    )
    whole = jnp.zeros((1, 1), jnp.float32)
    for t in range(steps):
        links = [load(space_ref.at[mu], t) for mu in range(3)]
        above = [load(above_ref.at[mu + 1], t) for mu in range(2)]

        def moved(mu, nu):
            if nu == 0:
                return mapped(step_x, links[mu])
            if nu == 1:
                return mapped(step_y, links[mu])
            return mapped(step_z, links[mu], above[mu])

        density = None
        for mu, nu in ((0, 1), (0, 2), (1, 2)):
            left = product(links[mu], moved(nu, mu))
            right = product(links[nu], moved(mu, nu))
            trace = None
            for i in range(3):
                for j in range(3):
                    term = left[i][j][0] * right[i][j][0] + left[i][j][1] * right[i][j][1]
                    trace = term if trace is None else trace + term
            term = 1.0 - trace / 3.0
            density = term if density is None else density + term
        prof = jnp.sum(density, axis=1, keepdims=True) / (3.0 * sites)
        row = jnp.sum(jnp.where(eye, jnp.broadcast_to(prof, (layers, layers)), 0.0), axis=0, keepdims=True)
        profile_ref[t : t + 1, :] = row
        whole = whole + jnp.sum(row, axis=1, keepdims=True)
    total_ref[...] = jnp.broadcast_to(whole, total_ref.shape)


def final_kernel(
    bit_ref, excl_ref, excl_up_ref, got_ref, got_up_ref, time_ref, time_up_ref, space_ref,
    gauge_ref, fixed_ref, up_ref,
):
    steps = time_ref.shape[3]
    upper = bit_ref[0] == 1

    @pl.when(upper)
    def _():
        store(gauge_ref, product(unpack(got_ref), load(excl_ref)), 0)
        store(up_ref, product(load(got_up_ref), load(excl_up_ref)))

    @pl.when(jnp.logical_not(upper))
    def _():
        store(gauge_ref, load(excl_ref), 0)
        store(up_ref, load(excl_up_ref))

    for t in range(steps):
        gauge = load(gauge_ref, t)
        above = load(up_ref)
        if t + 1 < steps:
            store(gauge_ref, product(gauge, load(time_ref, t)), t + 1)
            store(up_ref, product(above, load(time_up_ref.at[0], t)))
        for mu in range(3):
            if mu == 0:
                ahead = mapped(step_x, gauge)
            elif mu == 1:
                ahead = mapped(step_y, gauge)
            else:
                ahead = mapped(step_z, gauge, above)
            fixed = product_dagger(product(gauge, load(space_ref.at[mu], t)), ahead)
            store(fixed_ref.at[mu], fixed, t)


def call(kernel, out_shapes, args, smem=0, scratch=(), keep=()):
    return pl.pallas_call(
        kernel,
        out_shape=[
            pltpu.VMEM(s, jnp.float32) if i in keep else jax.ShapeDtypeStruct(s, jnp.float32)
            for i, s in enumerate(out_shapes)
        ],
        in_specs=[SMEM] * smem + [VMEM] * (len(args) - smem),
        out_specs=[VMEM] * len(out_shapes),
        scratch_shapes=list(scratch),
    )(*args)


def near(value):
    return pltpu.with_memory_space_constraint(value, pltpu.VMEM)


def make_on_device(n_ta, n_gz):
    both = ("ta", "gz")
    count = n_ta * n_gz
    bits = n_ta.bit_length() - 1

    def swap(value, axis, n, mask):
        return lax.ppermute(value, axis, [(i, i ^ mask) for i in range(n)])

    def from_upper(value, mask=0):
        pairs = [
            ((i ^ mask) * n_gz + (g + 1) % n_gz, i * n_gz + g) for i in range(n_ta) for g in range(n_gz)
        ]
        return lax.ppermute(value, both, pairs)

    def on_device(time_links, space_links):
        return body(time_links, space_links)

    def body(time_links, space_links):
        steps, layers, sites = time_links.shape[3:]
        mat = (2, 3, 3, layers, sites)
        packed = (14, layers, sites)
        low = (2, 3, 3, 1, sites)
        me = lax.axis_index("ta")

        def bit(at):
            return ((me >> at) & 1).reshape(1)

        def summed(part, masks):
            parts = [part, swap(part, both, count, masks[0]), swap(part, both, count, masks[1])]
            parts.append(swap(part, both, count, masks[0] ^ masks[1]))
            return (parts[0] + parts[1]) + (parts[2] + parts[3])

        space_near = near(space_links)
        total, lows = call(
            first_kernel,
            [packed, (3,) + time_links.shape[:4] + (1, sites)],
            [time_links, space_links],
            keep=(0, 1),
        )
        slots = [total]
        for mask in (1, 2, 3):
            slots.append(swap(total, "ta", n_ta, mask))
        lows_up = from_upper(lows)
        profile, part = call(
            plaquette_kernel,
            [(steps, layers), (1, 128)],
            [space_near, near(lows_up)],
            keep=(1,),
        )
        args = [(me & 3).reshape(1)] + [near(v) for v in slots]
        total, excl = call(
            functools.partial(group_kernel, 4), [packed, mat], args, 1, keep=range(2)
        )
        left = [1 << at for at in range(count.bit_length() - 1)]
        part = summed(part, left[:2])
        left = left[2:]
        for at in range(2, bits - 1):
            is_last = at == bits - 2
            other = swap(total, "ta", n_ta, 1 << at)
            args = [bit(at)] + [near(v) for v in (total, other, excl)]
            outs = call(
                functools.partial(combine_kernel, True, is_last),
                [packed, mat] + ([low, low] if is_last else []),
                args,
                1,
                keep=range(4),
            )
            total, excl = outs[0], outs[1]
        total_low, excl_low = outs[2], outs[3]
        top = 1 << (bits - 1)
        got = swap(total, "ta", n_ta, top)
        got_up = from_upper(total_low, top)
        excl_up = from_upper(excl_low)
        while len(left) > 1:
            part = summed(part, left[:2])
            left = left[2:]
        for mask in left:
            more = swap(part, both, count, mask)
            part = part + more
        args = [bit(bits - 1)] + [near(v) for v in (excl, excl_up, got, got_up)]
        args += [near(time_links), near(lows_up), space_near]
        gauge, fixed = call(
            final_kernel,
            [time_links.shape, space_links.shape],
            args,
            1,
            [pltpu.VMEM(low, jnp.float32)],
        )
        mean = part[0, 0] / (steps * layers * count)
        return gauge, fixed, profile, mean

    return on_device


def solution(mesh):
    return jax.shard_map(
        make_on_device(mesh.shape["ta"], mesh.shape["gz"]),
        mesh=mesh,
        in_specs=(
            P(None, None, None, "ta", "gz", None),
            P(None, None, None, None, "ta", "gz", None),
        ),
        out_specs=(
            P(None, None, None, "ta", "gz", None),
            P(None, None, None, None, "ta", "gz", None),
            P("ta", "gz"),
            P(),
        ),
        check_vma=False,
    )
```

```python
import functools

import jax
import jax.numpy as jnp
from jax import lax
from jax.experimental import pallas as pl
from jax.experimental.pallas import tpu as pltpu
from jax.sharding import PartitionSpec as P


Y = 16


VMEM = pl.BlockSpec(memory_space=pltpu.VMEM)
SMEM = pl.BlockSpec(memory_space=pltpu.SMEM)


def product(a, b):
    out = []
    for i in range(3):
        row = []
        for j in range(3):
            re = im = None
            for k in range(3):
                ar, ai = a[i][k]
                br, bi = b[k][j]
                r = ar * br - ai * bi
                m = ar * bi + ai * br
                re = r if re is None else re + r
                im = m if im is None else im + m
            row.append((re, im))
        out.append(row)
    return out


def product_dagger(a, b):
    out = []
    for i in range(3):
        row = []
        for j in range(3):
            re = im = None
            for k in range(3):
                ar, ai = a[i][k]
                br, bi = b[j][k]
                r = ar * br + ai * bi
                m = ai * br - ar * bi
                re = r if re is None else re + r
                im = m if im is None else im + m
            row.append((re, im))
        out.append(row)
    return out


def mapped(f, *mats):
    return [
        [tuple(f(*(m[i][j][c] for m in mats)) for c in range(2)) for j in range(3)]
        for i in range(3)
    ]


def load(ref, *tail):
    return [[tuple(ref[(c, i, j) + tail] for c in range(2)) for j in range(3)] for i in range(3)]


def store(ref, mat, *tail):
    for i in range(3):
        for j in range(3):
            for c in range(2):
                ref[(c, i, j) + tail] = mat[i][j][c]


def store_low(ref, mat):
    for i in range(3):
        for j in range(3):
            for c in range(2):
                ref[c, i, j] = mat[i][j][c][0:1, :]


def times(a, b):
    return a[0] * b[0] - a[1] * b[1], a[0] * b[1] + a[1] * b[0]


def cross(mat):
    out = []
    for j in range(3):
        k, m = (j + 1) % 3, (j + 2) % 3
        p = times(mat[0][k], mat[1][m])
        q = times(mat[0][m], mat[1][k])
        out.append((p[0] - q[0], p[1] - q[1]))
    return out


def pack(ref, mat):
    for i in range(2):
        for j in range(3):
            for c in range(2):
                ref[i * 6 + j * 2 + c] = mat[i][j][c]
    terms = [times(mat[2][j], v) for j, v in enumerate(cross(mat))]
    for c in range(2):
        ref[12 + c] = terms[0][c] + terms[1][c] + terms[2][c]


def unpack(ref):
    rows = [
        [tuple(ref[i * 6 + j * 2 + c] for c in range(2)) for j in range(3)] for i in range(2)
    ]
    det = (ref[12], ref[13])
    rows.append([times(det, (v[0], -v[1])) for v in cross(rows)])
    return rows


def step_x(v):
    return pltpu.roll(v, v.shape[-1] - Y, v.ndim - 1)


def step_y(v):
    n = v.shape[-1]
    lane = lax.broadcasted_iota(jnp.int32, v.shape, v.ndim - 1)
    last = lax.rem(lane, Y) == Y - 1
    ahead = pltpu.roll(v, n - 1, v.ndim - 1)
    back = pltpu.roll(v, Y - 1, v.ndim - 1)
    return jnp.where(last, back, ahead)


def step_z(v, above):
    return jnp.concatenate([v[1:, :], above], axis=0)


def first_kernel(time_ref, out_ref):
    steps = time_ref.shape[3]
    run = load(time_ref, 0)
    for t in range(1, steps):
        run = product(run, load(time_ref, t))
    pack(out_ref, run)


def low_kernel(time_ref, space_ref, low_ref):
    low_ref[0] = time_ref[..., 0:1, :]
    low_ref[1:3] = space_ref[0:2, ..., 0:1, :]


def group_kernel(radix, digit_ref, *refs):
    slots = refs[:radix]
    total_ref, excl_ref = refs[radix:]
    digit = digit_ref[0]
    for d in range(radix):

        @pl.when(digit == d)
        def _():
            run = None
            for j in range(radix):
                if j == d:
                    if run is None:
                        one = jnp.ones(excl_ref.shape[3:], jnp.float32)
                        zero = jnp.zeros_like(one)
                        excl = [[(one if a == b else zero, zero) for b in range(3)] for a in range(3)]
                        store(excl_ref, excl)
                    else:
                        store(excl_ref, run)
                piece = unpack(slots[j ^ d])
                run = piece if run is None else product(run, piece)
            pack(total_ref, run)


def combine_kernel(has_before, low, bit_ref, mine_ref, other_ref, *refs):
    before_ref = refs[0] if has_before else None
    outs = refs[1:] if has_before else refs
    total_ref, excl_ref = outs[0], outs[1]
    upper = bit_ref[0] == 1

    def finish(total, excl):
        pack(total_ref, total)
        store(excl_ref, excl)
        if low:
            store_low(outs[2], total)
            store_low(outs[3], excl)

    @pl.when(upper)
    def _():
        other = unpack(other_ref)
        excl = product(other, load(before_ref)) if has_before else other
        finish(product(other, unpack(mine_ref)), excl)

    @pl.when(jnp.logical_not(upper))
    def _():
        if has_before:
            excl = load(before_ref)
        else:
            one = jnp.ones(excl_ref.shape[3:], jnp.float32)
            zero = jnp.zeros_like(one)
            excl = [[(one if a == b else zero, zero) for b in range(3)] for a in range(3)]
        finish(product(unpack(mine_ref), unpack(other_ref)), excl)


def plaquette_kernel(space_ref, above_ref, profile_ref, total_ref):
    steps, layers = space_ref.shape[4], space_ref.shape[5]
    sites = space_ref.shape[6]
    eye = (
        lax.broadcasted_iota(jnp.int32, (layers, layers), 0)
        == lax.broadcasted_iota(jnp.int32, (layers, layers), 1)
    )
    whole = jnp.zeros((1, 1), jnp.float32)
    for t in range(steps):
        links = [load(space_ref.at[mu], t) for mu in range(3)]
        above = [load(above_ref.at[mu + 1], t) for mu in range(2)]

        def moved(mu, nu):
            if nu == 0:
                return mapped(step_x, links[mu])
            if nu == 1:
                return mapped(step_y, links[mu])
            return mapped(step_z, links[mu], above[mu])

        density = None
        for mu, nu in ((0, 1), (0, 2), (1, 2)):
            left = product(links[mu], moved(nu, mu))
            right = product(links[nu], moved(mu, nu))
            trace = None
            for i in range(3):
                for j in range(3):
                    term = left[i][j][0] * right[i][j][0] + left[i][j][1] * right[i][j][1]
                    trace = term if trace is None else trace + term
            term = 1.0 - trace / 3.0
            density = term if density is None else density + term
        prof = jnp.sum(density, axis=1, keepdims=True) / (3.0 * sites)
        row = jnp.sum(jnp.where(eye, jnp.broadcast_to(prof, (layers, layers)), 0.0), axis=0, keepdims=True)
        profile_ref[t : t + 1, :] = row
        whole = whole + jnp.sum(row, axis=1, keepdims=True)
    total_ref[...] = jnp.broadcast_to(whole, total_ref.shape)


def final_kernel(
    bit_ref, excl_ref, excl_up_ref, got_ref, got_up_ref, time_ref, time_up_ref, space_ref,
    gauge_ref, fixed_ref, up_ref,
):
    steps = time_ref.shape[3]
    upper = bit_ref[0] == 1

    @pl.when(upper)
    def _():
        store(gauge_ref, product(unpack(got_ref), load(excl_ref)), 0)
        store(up_ref, product(load(got_up_ref), load(excl_up_ref)))

    @pl.when(jnp.logical_not(upper))
    def _():
        store(gauge_ref, load(excl_ref), 0)
        store(up_ref, load(excl_up_ref))

    for t in range(steps):
        gauge = load(gauge_ref, t)
        above = load(up_ref)
        if t + 1 < steps:
            store(gauge_ref, product(gauge, load(time_ref, t)), t + 1)
            store(up_ref, product(above, load(time_up_ref.at[0], t)))
        for mu in range(3):
            if mu == 0:
                ahead = mapped(step_x, gauge)
            elif mu == 1:
                ahead = mapped(step_y, gauge)
            else:
                ahead = mapped(step_z, gauge, above)
            fixed = product_dagger(product(gauge, load(space_ref.at[mu], t)), ahead)
            store(fixed_ref.at[mu], fixed, t)


def call(kernel, out_shapes, args, smem=0, scratch=(), keep=()):
    return pl.pallas_call(
        kernel,
        out_shape=[
            pltpu.VMEM(s, jnp.float32) if i in keep else jax.ShapeDtypeStruct(s, jnp.float32)
            for i, s in enumerate(out_shapes)
        ],
        in_specs=[SMEM] * smem + [VMEM] * (len(args) - smem),
        out_specs=[VMEM] * len(out_shapes),
        scratch_shapes=list(scratch),
    )(*args)


def near(value):
    return pltpu.with_memory_space_constraint(value, pltpu.VMEM)


def make_on_device(n_ta, n_gz):
    both = ("ta", "gz")
    count = n_ta * n_gz
    bits = n_ta.bit_length() - 1

    def swap(value, axis, n, mask):
        return lax.ppermute(value, axis, [(i, i ^ mask) for i in range(n)])

    def from_upper(value, mask=0):
        pairs = [
            ((i ^ mask) * n_gz + (g + 1) % n_gz, i * n_gz + g) for i in range(n_ta) for g in range(n_gz)
        ]
        return lax.ppermute(value, both, pairs)

    def on_device(time_links, space_links):
        return body(time_links, space_links)

    def body(time_links, space_links):
        steps, layers, sites = time_links.shape[3:]
        mat = (2, 3, 3, layers, sites)
        packed = (14, layers, sites)
        low = (2, 3, 3, 1, sites)
        me = lax.axis_index("ta")

        def bit(at):
            return ((me >> at) & 1).reshape(1)

        def summed(part, masks):
            parts = [part, swap(part, both, count, masks[0]), swap(part, both, count, masks[1])]
            parts.append(swap(part, both, count, masks[0] ^ masks[1]))
            return (parts[0] + parts[1]) + (parts[2] + parts[3])

        space_near = near(space_links)
        total = call(first_kernel, [packed], [time_links], keep=(0,))[0]
        time_near = near(time_links)
        lows = call(
            low_kernel,
            [(3,) + time_links.shape[:4] + (1, sites)],
            [time_near, space_near],
            keep=(0,),
        )[0]
        slots = [total]
        for mask in (1, 2, 3):
            slots.append(swap(total, "ta", n_ta, mask))
        lows_up = from_upper(lows)
        profile, part = call(
            plaquette_kernel,
            [(steps, layers), (1, 128)],
            [space_near, near(lows_up)],
            keep=(1,),
        )
        args = [(me & 3).reshape(1)] + [near(v) for v in slots]
        total, excl = call(
            functools.partial(group_kernel, 4), [packed, mat], args, 1, keep=range(2)
        )
        left = [1 << at for at in range(count.bit_length() - 1)]
        part = summed(part, left[:2])
        left = left[2:]
        for at in range(2, bits - 1):
            is_last = at == bits - 2
            other = swap(total, "ta", n_ta, 1 << at)
            args = [bit(at)] + [near(v) for v in (total, other, excl)]
            outs = call(
                functools.partial(combine_kernel, True, is_last),
                [packed, mat] + ([low, low] if is_last else []),
                args,
                1,
                keep=range(4),
            )
            total, excl = outs[0], outs[1]
        total_low, excl_low = outs[2], outs[3]
        top = 3 << (bits - 2)
        got = swap(total, "ta", n_ta, top)
        got_up = from_upper(total_low, top)
        excl_up = from_upper(excl_low)
        while len(left) > 1:
            part = summed(part, left[:2])
            left = left[2:]
        for mask in left:
            more = swap(part, both, count, mask | mask >> 1)
            part = part + more
        args = [bit(bits - 1)] + [near(v) for v in (excl, excl_up, got, got_up)]
        args += [time_near, near(lows_up), space_near]
        gauge, fixed = call(
            final_kernel,
            [time_links.shape, space_links.shape],
            args,
            1,
            [pltpu.VMEM(low, jnp.float32)],
        )
        mean = part[0, 0] / (steps * layers * count)
        return gauge, fixed, profile, mean

    return on_device


def solution(mesh):
    return jax.shard_map(
        make_on_device(mesh.shape["ta"], mesh.shape["gz"]),
        mesh=mesh,
        in_specs=(
            P(None, None, None, "ta", "gz", None),
            P(None, None, None, None, "ta", "gz", None),
        ),
        out_specs=(
            P(None, None, None, "ta", "gz", None),
            P(None, None, None, None, "ta", "gz", None),
            P("ta", "gz"),
            P(),
        ),
        check_vma=False,
    )
```
